8 devices in a mesh: dp: 2 (over z, y), ctx: 4 (over x, core).
Axes of the slice: x: 2, y: 2, z: 1, core: 2. Of those that a mesh axis runs over, the one named last changes fastest.
Arguments:
- x_chunk: bfloat16 [6144, 2048], P(('dp', 'ctx')), parts along dimension 0
- cache_len: int32 [2], P('dp'), parts along dimension 0
- k_cache: bfloat16 [2, 16384, 16, 128], P(None, ('dp', 'ctx')), parts along dimension 1
- v_cache: bfloat16 [2, 16384, 16, 128], P(None, ('dp', 'ctx')), parts along dimension 1
- k_local: bfloat16 [2, 512, 16, 128], P(None, 'dp'), parts along dimension 1
- v_local: bfloat16 [2, 512, 16, 128], P(None, 'dp'), parts along dimension 1
- g_attn: bfloat16 [4, 2048], replicated
- g_mlp: bfloat16 [4, 2048], replicated
- w_q: bfloat16 [4, 2048, 2048], replicated
- w_k: bfloat16 [4, 2048, 2048], replicated
- w_v: bfloat16 [4, 2048, 2048], replicated
- w_o: bfloat16 [4, 2048, 2048], replicated
- w_gate: bfloat16 [4, 2048, 8192], replicated
- w_up: bfloat16 [4, 2048, 8192], replicated
- w_down: bfloat16 [4, 8192, 2048], replicated
Outputs:
- output: bfloat16 [6144, 2048], P(('dp', 'ctx')), parts along dimension 0
There are 2 independent parts. The reference program is written for one: setup_inputs(seed, part) draws one part's arguments, and reference() takes and returns one part's arrays. A program takes and returns all parts, laid end to end along the dimension named above; an argument that names none is the same for every part.
All inputs are finite; a program needn't handle non-finite values.
Results may differ from the reference program's by a relative error of at most 0.02.
Values are sent between devices in bfloat16 or wider.
A program may use at most 2.25 GiB of HBM per device.

```python
import math
import jax
import jax.numpy as jnp
from jax import lax

D_MODEL = 2048
NUM_HEADS = 16
KV_HEADS = 16
HEAD_DIM = 128
WINDOW = 256
FF_DIM = 8192
SEQ_NEW = 3072
CACHE_SIZE = 8192
QUERY_ROWS = 128
NUM_PAIRS = 2
NORM_EPS = 1e-6


def draw_normal(rng_key, arr_shape, factor):
    return jax.random.normal(rng_key, arr_shape, jnp.float32) * factor


def setup_inputs(seed: int = 0, part: int = 0) -> dict:
    part_keys = jax.random.split(jax.random.fold_in(jax.random.key(seed), part), 6)
    shared_keys = jax.random.split(jax.random.key(seed + 1), 9)
    n_layers = 2 * NUM_PAIRS
    q_width = NUM_HEADS * HEAD_DIM
    kv_width = KV_HEADS * HEAD_DIM
    gain_local = math.log(max(WINDOW / 8.0, 2.0)) ** 0.25
    gain_global = math.log(max((CACHE_SIZE + SEQ_NEW) / 16.0, 2.0)) ** 0.25
    gain_base = jnp.tile(jnp.array([gain_local, gain_global], jnp.float32), NUM_PAIRS)
    cache_shape = (NUM_PAIRS, CACHE_SIZE, KV_HEADS, HEAD_DIM)
    local_shape = (NUM_PAIRS, WINDOW, KV_HEADS, HEAD_DIM)
    x_chunk = draw_normal(part_keys[0], (SEQ_NEW, D_MODEL), 1.0).astype(jnp.bfloat16)
    cache_len = jax.random.randint(part_keys[1], (1,), CACHE_SIZE // 2, CACHE_SIZE + 1, jnp.int32)
    k_cache = draw_normal(part_keys[2], cache_shape, gain_global).astype(jnp.bfloat16)
    v_cache = draw_normal(part_keys[3], cache_shape, gain_global).astype(jnp.bfloat16)
    k_local = draw_normal(part_keys[4], local_shape, gain_local).astype(jnp.bfloat16)
    v_local = draw_normal(part_keys[5], local_shape, gain_local).astype(jnp.bfloat16)
    g_attn = (gain_base[:, None] * (1.0 + draw_normal(shared_keys[0], (n_layers, D_MODEL), 0.2))).astype(jnp.bfloat16)
    g_mlp = (1.0 + draw_normal(shared_keys[1], (n_layers, D_MODEL), 0.2)).astype(jnp.bfloat16)
    w_q = draw_normal(shared_keys[2], (n_layers, D_MODEL, q_width), D_MODEL ** -0.5).astype(jnp.bfloat16)
    w_k = draw_normal(shared_keys[3], (n_layers, D_MODEL, kv_width), D_MODEL ** -0.5).astype(jnp.bfloat16)
    w_v = draw_normal(shared_keys[4], (n_layers, D_MODEL, kv_width), D_MODEL ** -0.5).astype(jnp.bfloat16)
    w_o = draw_normal(shared_keys[5], (n_layers, q_width, D_MODEL), q_width ** -0.5).astype(jnp.bfloat16)
    w_gate = draw_normal(shared_keys[6], (n_layers, D_MODEL, FF_DIM), D_MODEL ** -0.5).astype(jnp.bfloat16)
    w_up = draw_normal(shared_keys[7], (n_layers, D_MODEL, FF_DIM), D_MODEL ** -0.5).astype(jnp.bfloat16)
    w_down = draw_normal(shared_keys[8], (n_layers, FF_DIM, D_MODEL), FF_DIM ** -0.5).astype(jnp.bfloat16)
    return {'x_chunk': x_chunk, 'cache_len': cache_len, 'k_cache': k_cache, 'v_cache': v_cache,
            'k_local': k_local, 'v_local': v_local, 'g_attn': g_attn, 'g_mlp': g_mlp,
            'w_q': w_q, 'w_k': w_k, 'w_v': w_v, 'w_o': w_o,
            'w_gate': w_gate, 'w_up': w_up, 'w_down': w_down}


def rms_norm(rows_in, gain_vec):
    rows_f32 = rows_in.astype(jnp.float32)
    inv_rms = lax.rsqrt(jnp.mean(rows_f32 * rows_f32, axis=-1, keepdims=True) + NORM_EPS)
    return (rows_f32 * inv_rms * gain_vec.astype(jnp.float32)).astype(jnp.bfloat16)


def project(rows_in, weight):
    return jnp.dot(rows_in, weight, preferred_element_type=jnp.float32).astype(jnp.bfloat16)


def qkv_heads(normed, w_query, w_key, w_value):
    groups = NUM_HEADS // KV_HEADS
    queries = project(normed, w_query).reshape(SEQ_NEW, KV_HEADS, groups, HEAD_DIM)
    new_k = project(normed, w_key).reshape(SEQ_NEW, KV_HEADS, HEAD_DIM)
    new_v = project(normed, w_value).reshape(SEQ_NEW, KV_HEADS, HEAD_DIM)
    return queries, new_k, new_v


def attend(score_list, value_list):
    row_max = score_list[0].max(axis=-1)
    for part_scores in score_list[1:]:
        row_max = jnp.maximum(row_max, part_scores.max(axis=-1))
    row_sum = 0.0
    weighted = 0.0
    for part_scores, part_values in zip(score_list, value_list):
        part_probs = jnp.exp(part_scores - row_max[..., None])
        row_sum = row_sum + part_probs.sum(axis=-1)
        weighted = weighted + jnp.einsum('hgqk,khd->qhgd', part_probs.astype(jnp.bfloat16).astype(jnp.float32), part_values.astype(jnp.float32))
    return (weighted / jnp.transpose(row_sum, (2, 0, 1))[..., None]).astype(jnp.bfloat16)


def local_attention(queries, ext_k, ext_v):
    score_scale = HEAD_DIM ** -0.5
    rel_pos = jnp.arange(WINDOW + QUERY_ROWS)[None, :] - jnp.arange(QUERY_ROWS)[:, None]
    band_mask = (rel_pos > 0) & (rel_pos <= WINDOW)

    def one_block(block_idx):
        row_start = block_idx * QUERY_ROWS
        q_rows = lax.dynamic_slice_in_dim(queries, row_start, QUERY_ROWS, axis=0).astype(jnp.float32)
        k_rows = lax.dynamic_slice_in_dim(ext_k, row_start, WINDOW + QUERY_ROWS, axis=0)
        v_rows = lax.dynamic_slice_in_dim(ext_v, row_start, WINDOW + QUERY_ROWS, axis=0)
        scores = jnp.einsum('qhgd,khd->hgqk', q_rows, k_rows.astype(jnp.float32)) * score_scale
        scores = jnp.where(band_mask, scores, -jnp.inf)
        return attend([scores], [v_rows])

    blocks = lax.map(one_block, jnp.arange(SEQ_NEW // QUERY_ROWS))
    return blocks.reshape(SEQ_NEW, NUM_HEADS * HEAD_DIM)


def global_attention(queries, cache_k, cache_v, new_k, new_v, valid_len):
    score_scale = HEAD_DIM ** -0.5
    cache_mask = jnp.arange(CACHE_SIZE) < valid_len
    new_pos = jnp.arange(SEQ_NEW)
    cache_f32 = cache_k.astype(jnp.float32)
    new_f32 = new_k.astype(jnp.float32)

    def one_block(block_idx):
        row_start = block_idx * QUERY_ROWS
        q_rows = lax.dynamic_slice_in_dim(queries, row_start, QUERY_ROWS, axis=0).astype(jnp.float32)
        q_pos = row_start + jnp.arange(QUERY_ROWS)
        cache_scores = jnp.einsum('qhgd,khd->hgqk', q_rows, cache_f32) * score_scale
        cache_scores = jnp.where(cache_mask, cache_scores, -jnp.inf)
        new_scores = jnp.einsum('qhgd,khd->hgqk', q_rows, new_f32) * score_scale
        new_scores = jnp.where(new_pos[None, :] <= q_pos[:, None], new_scores, -jnp.inf)
        return attend([cache_scores, new_scores], [cache_v, new_v])

    blocks = lax.map(one_block, jnp.arange(SEQ_NEW // QUERY_ROWS))
    return blocks.reshape(SEQ_NEW, NUM_HEADS * HEAD_DIM)


def add_residual(hidden, attn_out, w_out):
    return (hidden.astype(jnp.float32) + jnp.dot(attn_out, w_out, preferred_element_type=jnp.float32)).astype(jnp.bfloat16)


def mlp_block(hidden, gain_vec, w_gate, w_up, w_down):
    normed = rms_norm(hidden, gain_vec)
    gate_pre = jnp.dot(normed, w_gate, preferred_element_type=jnp.float32)
    up_pre = jnp.dot(normed, w_up, preferred_element_type=jnp.float32)
    act_bf16 = (jax.nn.gelu(gate_pre, approximate=True) * up_pre).astype(jnp.bfloat16)
    return (hidden.astype(jnp.float32) + jnp.dot(act_bf16, w_down, preferred_element_type=jnp.float32)).astype(jnp.bfloat16)


def reference(x_chunk, cache_len, k_cache, v_cache, k_local, v_local, g_attn, g_mlp, w_q, w_k, w_v, w_o, w_gate, w_up, w_down):
    hidden = x_chunk
    for pair_idx in range(NUM_PAIRS):
        layer_idx = 2 * pair_idx
        queries, new_k, new_v = qkv_heads(rms_norm(hidden, g_attn[layer_idx]), w_q[layer_idx], w_k[layer_idx], w_v[layer_idx])
        ext_k = jnp.concatenate([k_local[pair_idx], new_k], axis=0)
        ext_v = jnp.concatenate([v_local[pair_idx], new_v], axis=0)
        attn_out = local_attention(queries, ext_k, ext_v)
        hidden = add_residual(hidden, attn_out, w_o[layer_idx])
        hidden = mlp_block(hidden, g_mlp[layer_idx], w_gate[layer_idx], w_up[layer_idx], w_down[layer_idx])
        layer_idx = 2 * pair_idx + 1
        queries, new_k, new_v = qkv_heads(rms_norm(hidden, g_attn[layer_idx]), w_q[layer_idx], w_k[layer_idx], w_v[layer_idx])
        attn_out = global_attention(queries, k_cache[pair_idx], v_cache[pair_idx], new_k, new_v, cache_len[0])
        hidden = add_residual(hidden, attn_out, w_o[layer_idx])
        hidden = mlp_block(hidden, g_mlp[layer_idx], w_gate[layer_idx], w_up[layer_idx], w_down[layer_idx])
    return hidden
```

```python
import functools

import jax
import jax.numpy as jnp
from jax import lax
from jax.experimental import pallas as pl
from jax.experimental.pallas import tpu as pltpu
from jax.sharding import PartitionSpec as P

NORM_EPS = 1e-6
HEAD_DIM = 128
LOG2E = 1.4426950408889634
EXP_SCALE = LOG2E * HEAD_DIM ** -0.5
BLOCK_Q = 512
BLOCK_K = 1024
HALF_K = 512
NT = (((1,), (1,)), ((), ()))
TN = (((0,), (0,)), ((), ()))
ANY = pl.BlockSpec(memory_space=pl.ANY)


def rms_norm(rows_in, gain_vec):
    rows_f32 = rows_in.astype(jnp.float32)
    inv_rms = lax.rsqrt(jnp.mean(rows_f32 * rows_f32, axis=-1, keepdims=True) + NORM_EPS)
    return (rows_f32 * inv_rms * gain_vec.astype(jnp.float32)).astype(jnp.bfloat16)


def project(rows_in, weight):
    return jnp.dot(rows_in, weight, preferred_element_type=jnp.float32).astype(jnp.bfloat16)


def mlp_block(hidden, gain_vec, w_gate, w_up, w_down):
    normed = rms_norm(hidden, gain_vec)
    gate_pre = jnp.dot(normed, w_gate, preferred_element_type=jnp.float32)
    up_pre = jnp.dot(normed, w_up, preferred_element_type=jnp.float32)
    act_bf16 = (jax.nn.gelu(gate_pre, approximate=True) * up_pre).astype(jnp.bfloat16)
    return (hidden.astype(jnp.float32) + jnp.dot(act_bf16, w_down, preferred_element_type=jnp.float32)).astype(jnp.bfloat16)


def relay_kernel(me_ref, x_ref, *rest):
    outs, heads_s = rest[:-1], rest[-1]
    n_dev = len(outs)
    group = heads_s.shape[0] // n_dev
    me = me_ref[0]
    heads_s[...] = jnp.swapaxes(x_ref[...], 0, 1)
    for r, out in enumerate(outs):
        out[...] = heads_s[pl.ds(group * (me ^ r), group)]


def relay(me, cache, pair_idx, n_dev):
    _, slots, heads, dim = cache.shape
    rows = 512
    group = heads // n_dev
    return pl.pallas_call(
        relay_kernel,
        grid_spec=pltpu.PrefetchScalarGridSpec(
            num_scalar_prefetch=1,
            grid=(slots // rows,),
            in_specs=[pl.BlockSpec((None, rows, heads, dim), lambda i, m: (pair_idx, i, 0, 0))],
            out_specs=[pl.BlockSpec((group, rows, dim), lambda i, m: (0, i, 0))] * n_dev,
            scratch_shapes=[pltpu.VMEM((heads, rows, dim), cache.dtype)],
        ),
        out_shape=[jax.ShapeDtypeStruct((group, slots, dim), cache.dtype)] * n_dev,
        compiler_params=pltpu.CompilerParams(vmem_limit_bytes=40 << 20),
        cost_estimate=pl.CostEstimate(flops=0, bytes_accessed=4 * slots * heads * dim, transcendentals=0),
        name="cache_relay",
    )(me, cache)


def global_kernel(info_ref, q_ref, *rest, n_dev, slots, n_new):
    ck, cv = rest[:n_dev], rest[n_dev:2 * n_dev]
    nk, nv, o_ref, kbuf, vbuf, s0, s1, m_s, l_s, acc_s, sems = rest[2 * n_dev:]
    head, qi = pl.program_id(0), pl.program_id(1)
    n_heads = pl.num_programs(0)
    me, cache_len = info_ref[0], info_ref[1]
    n_cache = n_dev * slots

    def copies(h, slot):
        out = []
        for t, (pieces, new, buf) in enumerate(((ck, nk, kbuf), (cv, nv, vbuf))):
            for r in range(n_dev):
                dst = pl.multiple_of((me ^ r) * slots, slots)
                out.append(pltpu.make_async_copy(pieces[r].at[h], buf.at[slot, pl.ds(dst, slots)], sems.at[slot, t, r]))
            col = pl.multiple_of(h * HEAD_DIM, HEAD_DIM)
            out.append(pltpu.make_async_copy(new.at[:, pl.ds(col, HEAD_DIM)], buf.at[slot, pl.ds(n_cache, n_new)], sems.at[slot, t, n_dev]))
        return out

    slot = lax.rem(head, 2)

    @pl.when(qi == 0)
    def _():
        @pl.when(head == 0)
        def _():
            for c in copies(0, 0):
                c.start()

        @pl.when(head + 1 < n_heads)
        def _():
            for c in copies(head + 1, 1 - slot):
                c.start()

        for c in copies(head, slot):
            c.wait()

    q = q_ref[...]

    def scores(base, size):
        return lax.dot_general(kbuf[slot, pl.ds(base, size), :], q, NT, preferred_element_type=jnp.float32)

    def weigh(base, size, probs):
        return lax.dot_general(vbuf[slot, pl.ds(base, size), :], probs.astype(jnp.bfloat16), TN, preferred_element_type=jnp.float32)

    def update(base, s):
        m_old = m_s[...]
        m_new = jnp.maximum(m_old, jnp.max(s, axis=0, keepdims=True))
        alpha = jnp.exp2((m_old - m_new) * EXP_SCALE)
        probs = jnp.exp2((s - m_new) * EXP_SCALE)
        l_s[...] = l_s[...] * alpha + jnp.sum(probs, axis=0, keepdims=True)
        acc_s[...] = acc_s[...] * alpha + weigh(base, s.shape[0], probs)
        m_s[...] = m_new

    n_cache_full = cache_len // BLOCK_K
    n_new_full = qi // 2
    n_full = n_cache_full + n_new_full

    def base_of(j):
        b = jnp.where(j < n_cache_full, j * BLOCK_K, n_cache + (j - n_cache_full) * BLOCK_K)
        return pl.multiple_of(b, BLOCK_K)

    diag = pl.multiple_of(n_cache + qi * BLOCK_Q, BLOCK_Q)
    sd = scores(diag, BLOCK_Q)
    s0[...] = scores(base_of(0), BLOCK_K)
    key_ids = lax.broadcasted_iota(jnp.int32, sd.shape, 0)
    row_ids = lax.broadcasted_iota(jnp.int32, sd.shape, 1)
    sd = jnp.where(key_ids <= row_ids, sd, -jnp.inf)
    m_first = jnp.max(sd, axis=0, keepdims=True)
    pd = jnp.exp2((sd - m_first) * EXP_SCALE)
    l_s[...] = jnp.sum(pd, axis=0, keepdims=True)
    acc_s[...] = weigh(diag, BLOCK_Q, pd)
    m_s[...] = m_first

    @pl.when(lax.rem(qi, 2) == 1)
    def _():
        before = pl.multiple_of(n_cache + (qi - 1) * BLOCK_Q, BLOCK_Q)
        update(before, scores(before, HALF_K))

    def pair(i, carry):
        j = 2 * i
        s1[...] = scores(base_of(j + 1), BLOCK_K)
        update(base_of(j), s0[...])
        s0[...] = scores(base_of(jnp.minimum(j + 2, n_full - 1)), BLOCK_K)
        update(base_of(j + 1), s1[...])
        return carry

    lax.fori_loop(0, n_full // 2, pair, 0)

    @pl.when(lax.rem(n_full, 2) == 1)
    def _():
        update(base_of(n_full - 1), s0[...])

    @pl.when(lax.rem(cache_len, BLOCK_K) != 0)
    def _():
        last = pl.multiple_of(n_cache_full * BLOCK_K, BLOCK_K)
        s = scores(last, BLOCK_K)
        ids = last + lax.broadcasted_iota(jnp.int32, s.shape, 0)
        update(last, jnp.where(ids < cache_len, s, -jnp.inf))

    o_ref[...] = (acc_s[...] / l_s[...]).T.astype(jnp.bfloat16)


def global_attention(info, q, cache_k, cache_v, new_k, new_v):
    n_dev = len(cache_k)
    heads, slots, dim = cache_k[0].shape
    n_new = q.shape[0]
    n_keys = n_dev * slots + n_new
    elems = heads * n_new * (n_dev * slots * 3 // 4 + n_new // 2)
    return pl.pallas_call(
        functools.partial(global_kernel, n_dev=n_dev, slots=slots, n_new=n_new),
        grid_spec=pltpu.PrefetchScalarGridSpec(
            num_scalar_prefetch=1,
            grid=(heads, n_new // BLOCK_Q),
            in_specs=[pl.BlockSpec((BLOCK_Q, dim), lambda h, i, m: (i, h))] + [ANY] * (2 * n_dev + 2),
            out_specs=pl.BlockSpec((BLOCK_Q, dim), lambda h, i, m: (i, h)),
            scratch_shapes=[
                pltpu.VMEM((2, n_keys, dim), jnp.bfloat16),
                pltpu.VMEM((2, n_keys, dim), jnp.bfloat16),
                pltpu.VMEM((BLOCK_K, BLOCK_Q), jnp.float32),
                pltpu.VMEM((BLOCK_K, BLOCK_Q), jnp.float32),
                pltpu.VMEM((1, BLOCK_Q), jnp.float32),
                pltpu.VMEM((1, BLOCK_Q), jnp.float32),
                pltpu.VMEM((dim, BLOCK_Q), jnp.float32),
                pltpu.SemaphoreType.DMA((2, 2, n_dev + 1)),
            ],
        ),
        out_shape=jax.ShapeDtypeStruct((n_new, heads * dim), jnp.bfloat16),
        compiler_params=pltpu.CompilerParams(vmem_limit_bytes=56 << 20),
        cost_estimate=pl.CostEstimate(flops=8 * elems * dim, bytes_accessed=4 * heads * n_keys * dim, transcendentals=elems),
        name="global_attention",
    )(info, q, *cache_k, *cache_v, new_k, new_v)


def local_kernel(q_ref, k_ref, v_ref, hk_ref, hv_ref, o_ref, kbuf, vbuf, *, window):
    n_rows = q_ref.shape[0]
    dim = HEAD_DIM
    key_ids = lax.broadcasted_iota(jnp.int32, (2 * window, window), 0)
    row_ids = lax.broadcasted_iota(jnp.int32, (2 * window, window), 1)
    allowed = (key_ids > row_ids) & (key_ids <= row_ids + window)
    kbuf[pl.ds(0, window), :] = hk_ref[...]
    kbuf[pl.ds(window, n_rows), :] = k_ref[...]
    vbuf[pl.ds(0, window), :] = hv_ref[...]
    vbuf[pl.ds(window, n_rows), :] = v_ref[...]
    for h in range(q_ref.shape[1] // dim):
        cols = pl.ds(h * dim, dim)
        for b in range(n_rows // window):
            keys = pl.ds(b * window, 2 * window)
            rows = pl.ds(b * window, window)
            s = lax.dot_general(kbuf[keys, cols], q_ref[rows, cols], NT, preferred_element_type=jnp.float32)
            s = jnp.where(allowed, s, -jnp.inf)
            probs = jnp.exp2((s - jnp.max(s, axis=0, keepdims=True)) * EXP_SCALE)
            total = jnp.sum(probs, axis=0, keepdims=True)
            o = lax.dot_general(vbuf[keys, cols], probs.astype(jnp.bfloat16), TN, preferred_element_type=jnp.float32)
            o_ref[rows, cols] = (o / total).T.astype(jnp.bfloat16)


def local_attention(q, k, v, halo_k, halo_v):
    n_rows, width = q.shape
    window = halo_k.shape[0]
    cols = 512
    row_spec = pl.BlockSpec((n_rows, cols), lambda h: (0, h))
    halo_spec = pl.BlockSpec((window, cols), lambda h: (0, h))
    elems = n_rows * 2 * window * (width // HEAD_DIM)
    return pl.pallas_call(
        functools.partial(local_kernel, window=window),
        grid=(width // cols,),
        in_specs=[row_spec, row_spec, row_spec, halo_spec, halo_spec],
        out_specs=row_spec,
        out_shape=jax.ShapeDtypeStruct((n_rows, width), jnp.bfloat16),
        scratch_shapes=[pltpu.VMEM((window + n_rows, cols), jnp.bfloat16)] * 2,
        compiler_params=pltpu.CompilerParams(vmem_limit_bytes=32 << 20),
        cost_estimate=pl.CostEstimate(flops=8 * elems * HEAD_DIM, bytes_accessed=8 * n_rows * width, transcendentals=elems),
        name="local_attention",
    )(q, k, v, halo_k, halo_v)


def solution(mesh):
    n_dev = mesh.shape['ctx']
    shift_pairs = [(src_dev, src_dev + 1) for src_dev in range(n_dev - 1)]
    row_spec = P(('dp', 'ctx'), None)
    cache_spec = P(None, ('dp', 'ctx'), None, None)
    local_spec = P(None, 'dp', None, None)
    in_specs = (row_spec, P('dp'), cache_spec, cache_spec, local_spec, local_spec) + (P(),) * 9

    def exchange(pieces):
        out = [pieces[0]]
        for r in range(1, n_dev):
            out.append(lax.ppermute(pieces[r], 'ctx', [(d, d ^ r) for d in range(n_dev)]))
        return out

    def device_step(x_rows, cache_len, k_cache, v_cache, k_local, v_local, g_attn, g_mlp, w_q, w_k, w_v, w_o, w_gate, w_up, w_down):
        dev_idx = lax.axis_index('ctx')
        is_first = dev_idx == 0
        me = dev_idx.astype(jnp.int32).reshape(1)
        info = jnp.concatenate([me, cache_len])
        n_rows = x_rows.shape[0]
        pairs, window = k_local.shape[:2]
        width = w_q.shape[-1]
        group = width // n_dev
        halo_keys = k_local.reshape(pairs, window, width)
        halo_vals = v_local.reshape(pairs, window, width)

        cache_k, cache_v = [], []
        for p in range(pairs):
            cache_k.append(exchange(relay(me, k_cache, p, n_dev)))
            cache_v.append(exchange(relay(me, v_cache, p, n_dev)))

        hidden = x_rows
        for p in range(pairs):
            l = 2 * p
            h = rms_norm(hidden, g_attn[l])
            k, v = project(h, w_k[l]), project(h, w_v[l])
            halo_k = lax.ppermute(k[n_rows - window:], 'ctx', shift_pairs)
            halo_v = lax.ppermute(v[n_rows - window:], 'ctx', shift_pairs)
            q = project(h, w_q[l])
            halo_k = jnp.where(is_first, halo_keys[p], halo_k)
            halo_v = jnp.where(is_first, halo_vals[p], halo_v)
            attn = local_attention(q, k, v, halo_k, halo_v)
            hidden = (hidden.astype(jnp.float32) + jnp.dot(attn, w_o[l], preferred_element_type=jnp.float32)).astype(jnp.bfloat16)
            hidden = mlp_block(hidden, g_mlp[l], w_gate[l], w_up[l], w_down[l])

            l = 2 * p + 1
            h = rms_norm(hidden, g_attn[l])
            h_all = lax.all_gather(h, 'ctx', axis=0, tiled=True)
            q, k, v = [project(h_all, lax.dynamic_slice_in_dim(w[l], dev_idx * group, group, axis=1)) for w in (w_q, w_k, w_v)]
            o = global_attention(info, q, cache_k[p], cache_v[p], k, v)
            o = lax.all_to_all(o.reshape(n_dev, n_rows, group), 'ctx', 0, 0)
            attn_w = jnp.einsum('grc,gcd->rd', o, w_o[l].reshape(n_dev, group, -1), preferred_element_type=jnp.float32)
            hidden = (hidden.astype(jnp.float32) + attn_w).astype(jnp.bfloat16)
            hidden = mlp_block(hidden, g_mlp[l], w_gate[l], w_up[l], w_down[l])
        return hidden

    return jax.shard_map(device_step, mesh=mesh, in_specs=in_specs, out_specs=row_spec, check_vma=False)
```

```python
import functools

import jax
import jax.numpy as jnp
from jax import lax
from jax.experimental import pallas as pl
from jax.experimental.pallas import tpu as pltpu
from jax.sharding import PartitionSpec as P


NORM_EPS = 1e-6
HEAD_DIM = 128
LOG2E = 1.4426950408889634
EXP_SCALE = LOG2E * HEAD_DIM ** -0.5
BLOCK_K = 1024
NT = (((1,), (1,)), ((), ()))
TN = (((0,), (0,)), ((), ()))
ANY = pl.BlockSpec(memory_space=pl.ANY)


def rms_norm(rows_in, gain_vec):
    rows_f32 = rows_in.astype(jnp.float32)
    inv_rms = lax.rsqrt(jnp.mean(rows_f32 * rows_f32, axis=-1, keepdims=True) + NORM_EPS)
    return (rows_f32 * inv_rms * gain_vec.astype(jnp.float32)).astype(jnp.bfloat16)


def project(rows_in, weight):
    return jnp.dot(rows_in, weight, preferred_element_type=jnp.float32).astype(jnp.bfloat16)


def mlp_block(hidden, gain_vec, w_gate, w_up, w_down):
    normed = rms_norm(hidden, gain_vec)
    gate_pre = jnp.dot(normed, w_gate, preferred_element_type=jnp.float32)
    up_pre = jnp.dot(normed, w_up, preferred_element_type=jnp.float32)
    act_bf16 = (jax.nn.gelu(gate_pre, approximate=True) * up_pre).astype(jnp.bfloat16)
    return (hidden.astype(jnp.float32) + jnp.dot(act_bf16, w_down, preferred_element_type=jnp.float32)).astype(jnp.bfloat16)


def relay_kernel(me_ref, x_ref, *rest):
    outs, heads_s = rest[:-1], rest[-1]
    n_dev = len(outs)
    group = heads_s.shape[0] // n_dev
    me = me_ref[0]
    heads_s[...] = jnp.swapaxes(x_ref[...], 0, 1)
    for r, out in enumerate(outs):
        out[...] = heads_s[pl.ds(group * (me ^ r), group)]


def relay(me, cache, pair_idx, n_dev):
    _, slots, heads, dim = cache.shape
    rows = 512
    group = heads // n_dev
    return pl.pallas_call(
        relay_kernel,
        grid_spec=pltpu.PrefetchScalarGridSpec(
            num_scalar_prefetch=1,
            grid=(slots // rows,),
            in_specs=[pl.BlockSpec((None, rows, heads, dim), lambda i, m: (pair_idx, i, 0, 0))],
            out_specs=[pl.BlockSpec((group, rows, dim), lambda i, m: (0, i, 0))] * n_dev,
            scratch_shapes=[pltpu.VMEM((heads, rows, dim), cache.dtype)],
        ),
        out_shape=[jax.ShapeDtypeStruct((group, slots, dim), cache.dtype)] * n_dev,
        compiler_params=pltpu.CompilerParams(vmem_limit_bytes=40 << 20),
        cost_estimate=pl.CostEstimate(flops=0, bytes_accessed=4 * slots * heads * dim, transcendentals=0),
        name="cache_relay",
    )(me, cache)


def qkv_kernel(me_ref, h0_ref, h1_ref, wq_ref, wk_ref, wv_ref, q_ref, k_ref, v_ref):
    n_rows = h0_ref.shape[0]
    step = pl.program_id(0)
    for t, (w_ref, o_ref) in enumerate(((wq_ref, q_ref), (wk_ref, k_ref), (wv_ref, v_ref))):
        @pl.when(step // 2 == t)
        def _():
            for i, h_ref in enumerate((h0_ref, h1_ref)):
                o_ref[pl.ds(i * n_rows, n_rows), :] = jnp.dot(h_ref[...], w_ref[...], preferred_element_type=jnp.float32).astype(jnp.bfloat16)


def group_qkv(me, h0, h1, w_q, w_k, w_v, layer, n_dev):
    n_rows, depth = h0.shape
    group = w_q.shape[-1] // n_dev
    half = group // 2
    whole = pl.BlockSpec((n_rows, depth), lambda i, m: (0, 0))

    def w_spec(t):
        return pl.BlockSpec((None, depth, half), lambda i, m: (layer, 0, 2 * m[0] + jnp.clip(i - 2 * t, 0, 1)))

    def o_spec(t):
        return pl.BlockSpec((2 * n_rows, half), lambda i, m: (0, jnp.clip(i - 2 * t, 0, 1)))

    return pl.pallas_call(
        qkv_kernel,
        grid_spec=pltpu.PrefetchScalarGridSpec(
            num_scalar_prefetch=1,
            grid=(6,),
            in_specs=[whole, whole] + [w_spec(t) for t in range(3)],
            out_specs=[o_spec(t) for t in range(3)],
        ),
        out_shape=[jax.ShapeDtypeStruct((2 * n_rows, group), jnp.bfloat16)] * 3,
        compiler_params=pltpu.CompilerParams(vmem_limit_bytes=48 << 20),
        cost_estimate=pl.CostEstimate(flops=12 * n_rows * depth * group, bytes_accessed=4 * n_rows * depth + 6 * depth * group, transcendentals=0),
        name="group_qkv",
    )(me, h0, h1, w_q, w_k, w_v)


def out_kernel(me_ref, x_ref, o0, o1, o2, o3, w0, w1, w2, w3, y_ref):
    total = jnp.dot(o0[...], w0[...], preferred_element_type=jnp.float32)
    for o, w in ((o1, w1), (o2, w2), (o3, w3)):
        total = total + jnp.dot(o[...], w[...], preferred_element_type=jnp.float32)
    y_ref[...] = (x_ref[...].astype(jnp.float32) + total).astype(jnp.bfloat16)


def group_out(me, x, parts, w_o, layer):
    n_rows, width = x.shape
    group = parts[0].shape[1]
    cols = 512
    col_spec = pl.BlockSpec((n_rows, cols), lambda n, m: (0, n))
    part_spec = pl.BlockSpec((n_rows, group), lambda n, m: (0, 0))

    def w_spec(r):
        return pl.BlockSpec((None, group, cols), lambda n, m: (layer, m[0] ^ r, n))

    return pl.pallas_call(
        out_kernel,
        grid_spec=pltpu.PrefetchScalarGridSpec(
            num_scalar_prefetch=1,
            grid=(width // cols,),
            in_specs=[col_spec] + [part_spec] * 4 + [w_spec(r) for r in range(4)],
            out_specs=col_spec,
        ),
        out_shape=jax.ShapeDtypeStruct((n_rows, width), jnp.bfloat16),
        compiler_params=pltpu.CompilerParams(vmem_limit_bytes=48 << 20),
        cost_estimate=pl.CostEstimate(flops=2 * n_rows * width * width, bytes_accessed=2 * width * width, transcendentals=0),
        name="group_out",
    )(me, x, *parts, *([w_o] * 4))


def global_kernel(info_ref, q_ref, *rest, n_dev, slots, n_rows, first, use_cache, use_new, load, store):
    rest = list(rest)
    ck, cv = [[rest.pop(0) for _ in range(n_dev)] for _ in range(2)] if use_cache else ([], [])
    nk, nv = [[rest.pop(0) for _ in range(2)] for _ in range(2)] if use_new else ([], [])
    if load:
        m_in, l_in, acc_in = [rest.pop(0) for _ in range(3)]
    if store:
        m_out, l_out, acc_out = [rest.pop(0) for _ in range(3)]
    else:
        outs = [rest.pop(0) for _ in range(2)]
    kbuf, vbuf, s0, s1, qt, m_s, l_s, acc_s, sems = rest
    head, qi = pl.program_id(0), pl.program_id(1)
    n_heads = pl.num_programs(0)
    me, cache_len = info_ref[0], info_ref[1]
    n_cache = n_dev * slots if use_cache else 0

    def copies(h, slot):
        out = []
        col = pl.multiple_of(h * HEAD_DIM, HEAD_DIM)
        for t, (pieces, new, buf) in enumerate(((ck, nk, kbuf), (cv, nv, vbuf))):
            for r, piece in enumerate(pieces):
                dst = pl.multiple_of((me ^ r) * slots, slots)
                out.append(pltpu.make_async_copy(piece.at[h], buf.at[slot, pl.ds(dst, slots)], sems.at[slot, t, r]))
            for r in range(4 if use_new else 0):
                src = new[r // 2].at[pl.ds(n_rows * (r % 2), n_rows), pl.ds(col, HEAD_DIM)]
                dst = pl.multiple_of(n_cache + (me ^ r) * n_rows, 256)
                out.append(pltpu.make_async_copy(src, buf.at[slot, pl.ds(dst, n_rows)], sems.at[slot, t, n_dev + r]))
        return out

    slot = lax.rem(head, 2)

    @pl.when(qi == 0)
    def _():
        @pl.when(head == 0)
        def _():
            for c in copies(0, 0):
                c.start()

        @pl.when(head + 1 < n_heads)
        def _():
            for c in copies(head + 1, 1 - slot):
                c.start()

        for c in copies(head, slot):
            c.wait()

    qt[...] = q_ref[...].T
    if load:
        m_s[...], l_s[...], acc_s[...] = m_in[...], l_in[...], acc_in[...]
    else:
        m_s[...] = jnp.full_like(m_s, -jnp.inf)
        l_s[...] = jnp.zeros_like(l_s)
        acc_s[...] = jnp.zeros_like(acc_s)

    def scores(base, size):
        return jnp.dot(kbuf[slot, pl.ds(base, size), :], qt[...], preferred_element_type=jnp.float32)

    def update(base, s):
        size = s.shape[0]
        m_old = m_s[...]
        m_new = jnp.maximum(m_old, jnp.max(s, axis=0, keepdims=True))
        alpha = jnp.exp2((m_old - m_new) * EXP_SCALE)
        probs = jnp.exp2((s - m_new) * EXP_SCALE)
        l_s[...] = l_s[...] * alpha + jnp.sum(probs, axis=0, keepdims=True)
        weighted = lax.dot_general(vbuf[slot, pl.ds(base, size), :], probs.astype(jnp.bfloat16), TN, preferred_element_type=jnp.float32)
        acc_s[...] = acc_s[...] * alpha + weighted
        m_s[...] = m_new

    if use_cache:
        last = n_cache // BLOCK_K - 1
        n_full = cache_len // BLOCK_K
        n_left = cache_len - n_full * BLOCK_K

        def base_of(j):
            return pl.multiple_of(jnp.minimum(j, last) * BLOCK_K, BLOCK_K)

        def update_last(s):
            ids = lax.broadcasted_iota(jnp.int32, s.shape, 0)
            update(base_of(n_full), jnp.where(ids < n_left, s, -jnp.inf))

        s0[...] = scores(0, BLOCK_K)

        def pair(i, carry):
            j = 2 * i
            s1[...] = scores(base_of(j + 1), BLOCK_K)
            update(base_of(j), s0[...])
            s0[...] = scores(base_of(j + 2), BLOCK_K)
            update(base_of(j + 1), s1[...])
            return carry

        lax.fori_loop(0, n_full // 2, pair, 0)
        odd = lax.rem(n_full, 2) == 1

        @pl.when(odd)
        def _():
            s1[...] = scores(base_of(n_full), BLOCK_K)
            update(base_of(n_full - 1), s0[...])

            @pl.when(n_left > 0)
            def _():
                update_last(s1[...])

        @pl.when(jnp.logical_not(odd) & (n_left > 0))
        def _():
            update_last(s0[...])

    if use_new:
        piece = me ^ (first + qi)

        def new_base(j):
            return pl.multiple_of(n_cache + j * n_rows, 256)

        def earlier(j, carry):
            update(new_base(j), scores(new_base(j), n_rows))
            return carry

        lax.fori_loop(0, piece, earlier, 0)
        s = scores(new_base(piece), n_rows)
        key_ids = lax.broadcasted_iota(jnp.int32, s.shape, 0)
        row_ids = lax.broadcasted_iota(jnp.int32, s.shape, 1)
        update(new_base(piece), jnp.where(key_ids <= row_ids, s, -jnp.inf))

    if store:
        m_out[...], l_out[...], acc_out[...] = m_s[...], l_s[...], acc_s[...]
    else:
        result = (acc_s[...] / l_s[...]).T.astype(jnp.bfloat16)
        for i, o_ref in enumerate(outs):
            @pl.when(qi == i)
            def _():
                o_ref[...] = result


def global_attention(info, q, cache_k=(), cache_v=(), new_k=(), new_v=(), state=(), first=0, store=False, n_dev=4):
    dim = HEAD_DIM
    n_rows, group = q.shape[0] // 2, q.shape[1]
    heads = group // dim
    slots = cache_k[0].shape[1] if cache_k else 0
    n_keys = n_dev * (slots + (n_rows if new_k else 0))
    elems = heads * 2 * n_rows * (n_dev * slots * 3 // 4 + (n_dev * n_rows // 2 if new_k else 0))
    state_specs = [pl.BlockSpec((None, None, r, n_rows), lambda h, i, m: (h, i, 0, 0)) for r in (1, 1, dim)]
    state_shape = [jax.ShapeDtypeStruct((heads, 2, r, n_rows), jnp.float32) for r in (1, 1, dim)]
    return pl.pallas_call(
        functools.partial(global_kernel, n_dev=n_dev, slots=slots, n_rows=n_rows, first=first, use_cache=bool(cache_k), use_new=bool(new_k), load=bool(state), store=store),
        grid_spec=pltpu.PrefetchScalarGridSpec(
            num_scalar_prefetch=1,
            grid=(heads, 2),
            in_specs=[pl.BlockSpec((n_rows, dim), lambda h, i, m: (i, h))] + [ANY] * (2 * len(cache_k) + 2 * len(new_k)) + (state_specs if state else []),
            out_specs=state_specs if store else [pl.BlockSpec((n_rows, dim), lambda h, i, m: (0, h))] * 2,
            scratch_shapes=[
                pltpu.VMEM((2, n_keys, dim), jnp.bfloat16),
                pltpu.VMEM((2, n_keys, dim), jnp.bfloat16),
                pltpu.VMEM((BLOCK_K, n_rows), jnp.float32),
                pltpu.VMEM((BLOCK_K, n_rows), jnp.float32),
                pltpu.VMEM((dim, n_rows), jnp.bfloat16),
                pltpu.VMEM((1, n_rows), jnp.float32),
                pltpu.VMEM((1, n_rows), jnp.float32),
                pltpu.VMEM((dim, n_rows), jnp.float32),
                pltpu.SemaphoreType.DMA((2, 2, n_dev + 4)),
            ],
        ),
        out_shape=state_shape if store else [jax.ShapeDtypeStruct((n_rows, group), jnp.bfloat16)] * 2,
        compiler_params=pltpu.CompilerParams(vmem_limit_bytes=56 << 20),
        cost_estimate=pl.CostEstimate(flops=8 * elems * dim, bytes_accessed=4 * heads * n_keys * dim, transcendentals=elems),
        name="global_attention",
    )(info, q, *cache_k, *cache_v, *new_k, *new_v, *state)


def local_kernel(q_ref, k_ref, v_ref, hk_ref, hv_ref, o_ref, kbuf, vbuf, *, window):
    n_rows = q_ref.shape[0]
    dim = HEAD_DIM
    key_ids = lax.broadcasted_iota(jnp.int32, (2 * window, window), 0)
    row_ids = lax.broadcasted_iota(jnp.int32, (2 * window, window), 1)
    allowed = (key_ids > row_ids) & (key_ids <= row_ids + window)
    kbuf[pl.ds(0, window), :] = hk_ref[...]
    kbuf[pl.ds(window, n_rows), :] = k_ref[...]
    vbuf[pl.ds(0, window), :] = hv_ref[...]
    vbuf[pl.ds(window, n_rows), :] = v_ref[...]
    for h in range(q_ref.shape[1] // dim):
        cols = pl.ds(h * dim, dim)
        for b in range(n_rows // window):
            keys = pl.ds(b * window, 2 * window)
            rows = pl.ds(b * window, window)
            s = lax.dot_general(kbuf[keys, cols], q_ref[rows, cols], NT, preferred_element_type=jnp.float32)
            s = jnp.where(allowed, s, -jnp.inf)
            probs = jnp.exp2((s - jnp.max(s, axis=0, keepdims=True)) * EXP_SCALE)
            total = jnp.sum(probs, axis=0, keepdims=True)
            o = lax.dot_general(vbuf[keys, cols], probs.astype(jnp.bfloat16), TN, preferred_element_type=jnp.float32)
            o_ref[rows, cols] = (o / total).T.astype(jnp.bfloat16)


def local_attention(q, k, v, halo_k, halo_v):
    n_rows, width = q.shape
    window = halo_k.shape[0]
    cols = 512
    row_spec = pl.BlockSpec((n_rows, cols), lambda h: (0, h))
    halo_spec = pl.BlockSpec((window, cols), lambda h: (0, h))
    elems = n_rows * 2 * window * (width // HEAD_DIM)
    return pl.pallas_call(
        functools.partial(local_kernel, window=window),
        grid=(width // cols,),
        in_specs=[row_spec, row_spec, row_spec, halo_spec, halo_spec],
        out_specs=row_spec,
        out_shape=jax.ShapeDtypeStruct((n_rows, width), jnp.bfloat16),
        scratch_shapes=[pltpu.VMEM((window + n_rows, cols), jnp.bfloat16)] * 2,
        compiler_params=pltpu.CompilerParams(vmem_limit_bytes=32 << 20),
        cost_estimate=pl.CostEstimate(flops=8 * elems * HEAD_DIM, bytes_accessed=8 * n_rows * width, transcendentals=elems),
        name="local_attention",
    )(q, k, v, halo_k, halo_v)


def solution(mesh):
    n_dev = mesh.shape['ctx']
    shift_pairs = [(src_dev, src_dev + 1) for src_dev in range(n_dev - 1)]
    row_spec = P(('dp', 'ctx'), None)
    cache_spec = P(None, ('dp', 'ctx'), None, None)
    local_spec = P(None, 'dp', None, None)
    in_specs = (row_spec, P('dp'), cache_spec, cache_spec, local_spec, local_spec) + (P(),) * 9

    def swap(x, r):
        return lax.ppermute(x, 'ctx', [(d, d ^ r) for d in range(n_dev)])

    def device_step(x_rows, cache_len, k_cache, v_cache, k_local, v_local, g_attn, g_mlp, w_q, w_k, w_v, w_o, w_gate, w_up, w_down):
        dev_idx = lax.axis_index('ctx')
        is_first = dev_idx == 0
        me = dev_idx.astype(jnp.int32).reshape(1)
        info = jnp.concatenate([me, cache_len])
        n_rows = x_rows.shape[0]
        pairs, window = k_local.shape[:2]
        width = w_q.shape[-1]
        halo_keys = k_local.reshape(pairs, window, width)
        halo_vals = v_local.reshape(pairs, window, width)
        sent = {}

        def relay_both(p):
            return relay(me, k_cache, p, n_dev), relay(me, v_cache, p, n_dev)

        def send(p, t, pieces):
            sent[p, t] = [pieces[0]] + [swap(pieces[r], r) for r in (1, 2, 3)]

        k_pieces, v_pieces = relay_both(0)
        x_rows, k_pieces = lax.optimization_barrier((x_rows, k_pieces))
        send(0, 'k', k_pieces)
        send(0, 'v', v_pieces)

        hidden = x_rows
        for p in range(pairs):
            l = 2 * p
            h = rms_norm(hidden, g_attn[l])
            k = project(h, w_k[l])
            v = project(h, w_v[l])
            halo_k = lax.ppermute(k[n_rows - window:], 'ctx', shift_pairs)
            halo_v = lax.ppermute(v[n_rows - window:], 'ctx', shift_pairs)
            q = project(h, w_q[l])
            halo_k = jnp.where(is_first, halo_keys[p], halo_k)
            halo_v = jnp.where(is_first, halo_vals[p], halo_v)
            attn = local_attention(q, k, v, halo_k, halo_v)
            hidden = (hidden.astype(jnp.float32) + jnp.dot(attn, w_o[l], preferred_element_type=jnp.float32)).astype(jnp.bfloat16)
            hidden = mlp_block(hidden, g_mlp[l], w_gate[l], w_up[l], w_down[l])

            l = 2 * p + 1
            h = rms_norm(hidden, g_attn[l])
            h1 = swap(h, 1)
            h2 = swap(h, 2)
            q_near, k_near, v_near = group_qkv(me, h, h1, w_q, w_k, w_v, l, n_dev)
            state = global_attention(info, q_near, sent[p, 'k'], sent[p, 'v'], store=True)
            h3 = swap(h2, 1)
            q_far, k_far, v_far = group_qkv(me, h2, h3, w_q, w_k, w_v, l, n_dev)
            if p + 1 < pairs:
                k_pieces, v_pieces = relay_both(p + 1)
                k_pieces, v_pieces = lax.optimization_barrier((k_pieces, v_pieces, q_far))[:2]
                send(p + 1, 'k', k_pieces)
            o2, o3 = global_attention(info, q_far, sent[p, 'k'], sent[p, 'v'], (k_near, k_far), (v_near, v_far), first=2)
            o2, o3 = swap(o2, 2), swap(o3, 3)
            if p + 1 < pairs:
                send(p + 1, 'v', v_pieces)
            o0, o1 = global_attention(info, q_near, (), (), (k_near, k_far), (v_near, v_far), state)
            o1 = swap(o1, 1)
            hidden = group_out(me, hidden, (o0, o1, o2, o3), w_o, l)
            hidden = mlp_block(hidden, g_mlp[l], w_gate[l], w_up[l], w_down[l])
        return hidden

    return jax.shard_map(device_step, mesh=mesh, in_specs=in_specs, out_specs=row_spec, check_vma=False)
```

```python
import functools

import jax
import jax.numpy as jnp
from jax import lax
from jax.experimental import pallas as pl
from jax.experimental.pallas import tpu as pltpu
from jax.sharding import PartitionSpec as P


NORM_EPS = 1e-6
HEAD_DIM = 128
LOG2E = 1.4426950408889634
EXP_SCALE = LOG2E * HEAD_DIM ** -0.5
BLOCK_K = 1024
NT = (((1,), (1,)), ((), ()))
TN = (((0,), (0,)), ((), ()))
ANY = pl.BlockSpec(memory_space=pl.ANY)


def rms_norm(rows_in, gain_vec):
    rows_f32 = rows_in.astype(jnp.float32)
    inv_rms = lax.rsqrt(jnp.mean(rows_f32 * rows_f32, axis=-1, keepdims=True) + NORM_EPS)
    return (rows_f32 * inv_rms * gain_vec.astype(jnp.float32)).astype(jnp.bfloat16)


def project(rows_in, weight):
    return jnp.dot(rows_in, weight, preferred_element_type=jnp.float32).astype(jnp.bfloat16)


def relay_kernel(me_ref, x_ref, *rest):
    outs, heads_s = rest[:-1], rest[-1]
    n_dev = len(outs)
    group = heads_s.shape[0] // n_dev
    me = me_ref[0]
    heads_s[...] = jnp.swapaxes(x_ref[...], 0, 1)
    for r, out in enumerate(outs):
        out[...] = heads_s[pl.ds(group * (me ^ r), group)]


def relay(me, cache, pair_idx, n_dev):
    _, slots, heads, dim = cache.shape
    rows = 512
    group = heads // n_dev
    return pl.pallas_call(
        relay_kernel,
        grid_spec=pltpu.PrefetchScalarGridSpec(
            num_scalar_prefetch=1,
            grid=(slots // rows,),
            in_specs=[pl.BlockSpec((None, rows, heads, dim), lambda i, m: (pair_idx, i, 0, 0))],
            out_specs=[pl.BlockSpec((group, rows, dim), lambda i, m: (0, i, 0))] * n_dev,
            scratch_shapes=[pltpu.VMEM((heads, rows, dim), cache.dtype)],
        ),
        out_shape=[jax.ShapeDtypeStruct((group, slots, dim), cache.dtype)] * n_dev,
        compiler_params=pltpu.CompilerParams(vmem_limit_bytes=40 << 20),
        cost_estimate=pl.CostEstimate(flops=0, bytes_accessed=4 * slots * heads * dim, transcendentals=0),
        name="cache_relay",
    )(me, cache)


def qkv_kernel(me_ref, h0_ref, h1_ref, wq_ref, wk_ref, wv_ref, q_ref, k_ref, v_ref):
    n_rows = h0_ref.shape[0]
    step = pl.program_id(0)
    for t, (w_ref, o_ref) in enumerate(((wq_ref, q_ref), (wk_ref, k_ref), (wv_ref, v_ref))):
        @pl.when(step // 2 == t)
        def _():
            for i, h_ref in enumerate((h0_ref, h1_ref)):
                o_ref[pl.ds(i * n_rows, n_rows), :] = jnp.dot(h_ref[...], w_ref[...], preferred_element_type=jnp.float32).astype(jnp.bfloat16)


def group_qkv(me, h0, h1, w_q, w_k, w_v, layer, n_dev):
    n_rows, depth = h0.shape
    group = w_q.shape[-1] // n_dev
    half = group // 2
    whole = pl.BlockSpec((n_rows, depth), lambda i, m: (0, 0))

    def w_spec(t):
        return pl.BlockSpec((None, depth, half), lambda i, m: (layer, 0, 2 * m[0] + jnp.clip(i - 2 * t, 0, 1)))

    def o_spec(t):
        return pl.BlockSpec((2 * n_rows, half), lambda i, m: (0, jnp.clip(i - 2 * t, 0, 1)))

    return pl.pallas_call(
        qkv_kernel,
        grid_spec=pltpu.PrefetchScalarGridSpec(
            num_scalar_prefetch=1,
            grid=(6,),
            in_specs=[whole, whole] + [w_spec(t) for t in range(3)],
            out_specs=[o_spec(t) for t in range(3)],
        ),
        out_shape=[jax.ShapeDtypeStruct((2 * n_rows, group), jnp.bfloat16)] * 3,
        compiler_params=pltpu.CompilerParams(vmem_limit_bytes=48 << 20),
        cost_estimate=pl.CostEstimate(flops=12 * n_rows * depth * group, bytes_accessed=4 * n_rows * depth + 6 * depth * group, transcendentals=0),
        name="group_qkv",
    )(me, h0, h1, w_q, w_k, w_v)


def norm_rows(x, gain_ref):
    inv_rms = lax.rsqrt(jnp.mean(x * x, axis=-1, keepdims=True) + NORM_EPS)
    return (x * inv_rms * gain_ref[...].astype(jnp.float32)).astype(jnp.bfloat16)


def mlp_kernel(me_ref, x_ref, *rest, n_parts, n_out, n_mlp, with_next):
    rest = list(rest)
    parts = [rest.pop(0) for _ in range(n_parts)]
    w_parts = [rest.pop(0) for _ in range(n_parts)]
    gain, wg_ref, wu_ref, wd_ref = [rest.pop(0) for _ in range(4)]
    next_gain = rest.pop(0) if with_next else None
    y_ref = rest.pop(0)
    next_ref = rest.pop(0) if with_next else None
    acc, h_s = rest
    step = pl.program_id(0)
    cols = x_ref.shape[1]

    @pl.when(step < n_out)
    def _():
        total = x_ref[...].astype(jnp.float32)
        attn = jnp.dot(parts[0][...], w_parts[0][...], preferred_element_type=jnp.float32)
        for o, w in zip(parts[1:], w_parts[1:]):
            attn = attn + jnp.dot(o[...], w[...], preferred_element_type=jnp.float32)
        acc[:, pl.ds(pl.multiple_of(step * cols, cols), cols)] = (total + attn).astype(jnp.bfloat16).astype(jnp.float32)

    @pl.when(step == n_out - 1)
    def _():
        h_s[...] = norm_rows(acc[...], gain)

    @pl.when(step >= n_out)
    def _():
        h = h_s[...]
        gate = jnp.dot(h, wg_ref[...], preferred_element_type=jnp.float32)
        up = jnp.dot(h, wu_ref[...], preferred_element_type=jnp.float32)
        act = (jax.nn.gelu(gate, approximate=True) * up).astype(jnp.bfloat16)
        acc[...] += jnp.dot(act, wd_ref[...], preferred_element_type=jnp.float32)

    @pl.when(step == n_out + n_mlp - 1)
    def _():
        y = acc[...].astype(jnp.bfloat16)
        y_ref[...] = y
        if with_next:
            next_ref[...] = norm_rows(y.astype(jnp.float32), next_gain)


def out_mlp(me, x, parts, w_o, gains, w_gate, w_up, w_down, layer, next_gains=None):
    n_rows, width = x.shape
    depth = w_gate.shape[-1]
    cols, block = 512, 512
    n_out, n_mlp = width // cols, depth // block
    group = width // len(parts)
    with_next = next_gains is not None

    def out_step(i):
        return jnp.minimum(i, n_out - 1)

    def mlp_step(i):
        return jnp.maximum(i - n_out, 0)

    def part_w(r):
        if len(parts) == 1:
            return pl.BlockSpec((None, width, cols), lambda i, m: (layer, 0, out_step(i)))
        return pl.BlockSpec((None, group, cols), lambda i, m: (layer, m[0] ^ r, out_step(i)))

    whole = pl.BlockSpec((n_rows, width), lambda i, m: (0, 0))
    in_specs = (
        [pl.BlockSpec((n_rows, cols), lambda i, m: (0, out_step(i)))]
        + [pl.BlockSpec((n_rows, group), lambda i, m: (0, 0))] * len(parts)
        + [part_w(r) for r in range(len(parts))]
        + [pl.BlockSpec((None, 1, width), lambda i, m: (layer, 0, 0))]
        + [pl.BlockSpec((None, width, block), lambda i, m: (layer, 0, mlp_step(i)))] * 2
        + [pl.BlockSpec((None, block, width), lambda i, m: (layer, mlp_step(i), 0))]
    )
    args = [x, *parts, *([w_o] * len(parts)), gains, w_gate, w_up, w_down]
    if with_next:
        in_specs.append(pl.BlockSpec((None, 1, width), lambda i, m: (layer + 1, 0, 0)))
        args.append(next_gains)
    n_res = 1 + with_next
    res = pl.pallas_call(
        functools.partial(mlp_kernel, n_parts=len(parts), n_out=n_out, n_mlp=n_mlp, with_next=with_next),
        grid_spec=pltpu.PrefetchScalarGridSpec(
            num_scalar_prefetch=1,
            grid=(n_out + n_mlp,),
            in_specs=in_specs,
            out_specs=[whole] * n_res,
            scratch_shapes=[pltpu.VMEM((n_rows, width), jnp.float32), pltpu.VMEM((n_rows, width), jnp.bfloat16)],
        ),
        out_shape=[jax.ShapeDtypeStruct((n_rows, width), jnp.bfloat16)] * n_res,
        compiler_params=pltpu.CompilerParams(vmem_limit_bytes=62 << 20),
        cost_estimate=pl.CostEstimate(flops=2 * n_rows * width * (width + 3 * depth), bytes_accessed=2 * width * (width + 3 * depth), transcendentals=n_rows * depth),
        name="out_mlp",
    )(me, *args)
    return res if with_next else res[0]


def global_kernel(info_ref, q_ref, *rest, n_dev, slots, n_rows, first, use_cache, use_new, load, store):
    rest = list(rest)
    ck, cv = [[rest.pop(0) for _ in range(n_dev)] for _ in range(2)] if use_cache else ([], [])
    nk, nv = [[rest.pop(0) for _ in range(2)] for _ in range(2)] if use_new else ([], [])
    if load:
        m_in, l_in, acc_in = [rest.pop(0) for _ in range(3)]
    if store:
        m_out, l_out, acc_out = [rest.pop(0) for _ in range(3)]
    else:
        outs = [rest.pop(0) for _ in range(2)]
    kbuf, vbuf, s0, s1, qt, m_s, l_s, acc_s, sems = rest
    head, qi = pl.program_id(0), pl.program_id(1)
    n_heads = pl.num_programs(0)
    me, cache_len = info_ref[0], info_ref[1]
    n_cache = n_dev * slots if use_cache else 0

    def copies(h, slot):
        out = []
        col = pl.multiple_of(h * HEAD_DIM, HEAD_DIM)
        for t, (pieces, new, buf) in enumerate(((ck, nk, kbuf), (cv, nv, vbuf))):
            for r, piece in enumerate(pieces):
                dst = pl.multiple_of((me ^ r) * slots, slots)
                out.append(pltpu.make_async_copy(piece.at[h], buf.at[slot, pl.ds(dst, slots)], sems.at[slot, t, r]))
            for r in range(4 if use_new else 0):
                src = new[r // 2].at[pl.ds(n_rows * (r % 2), n_rows), pl.ds(col, HEAD_DIM)]
                dst = pl.multiple_of(n_cache + (me ^ r) * n_rows, 256)
                out.append(pltpu.make_async_copy(src, buf.at[slot, pl.ds(dst, n_rows)], sems.at[slot, t, n_dev + r]))
        return out

    slot = lax.rem(head, 2)

    @pl.when(qi == 0)
    def _():
        @pl.when(head == 0)
        def _():
            for c in copies(0, 0):
                c.start()

        @pl.when(head + 1 < n_heads)
        def _():
            for c in copies(head + 1, 1 - slot):
                c.start()

        for c in copies(head, slot):
            c.wait()

    qt[...] = q_ref[...].T
    if load:
        m_s[...], l_s[...], acc_s[...] = m_in[...], l_in[...], acc_in[...]
    else:
        m_s[...] = jnp.full_like(m_s, -jnp.inf)
        l_s[...] = jnp.zeros_like(l_s)
        acc_s[...] = jnp.zeros_like(acc_s)

    def scores(base, size):
        return jnp.dot(kbuf[slot, pl.ds(base, size), :], qt[...], preferred_element_type=jnp.float32)

    def update(base, s):
        size = s.shape[0]
        m_old = m_s[...]
        m_new = jnp.maximum(m_old, jnp.max(s, axis=0, keepdims=True))
        alpha = jnp.exp2((m_old - m_new) * EXP_SCALE)
        probs = jnp.exp2((s - m_new) * EXP_SCALE)
        l_s[...] = l_s[...] * alpha + jnp.sum(probs, axis=0, keepdims=True)
        weighted = lax.dot_general(vbuf[slot, pl.ds(base, size), :], probs.astype(jnp.bfloat16), TN, preferred_element_type=jnp.float32)
        acc_s[...] = acc_s[...] * alpha + weighted
        m_s[...] = m_new

    if use_cache:
        last = n_cache // BLOCK_K - 1
        n_full = cache_len // BLOCK_K
        n_left = cache_len - n_full * BLOCK_K

        def base_of(j):
            return pl.multiple_of(jnp.minimum(j, last) * BLOCK_K, BLOCK_K)

        def update_last(s):
            ids = lax.broadcasted_iota(jnp.int32, s.shape, 0)
            update(base_of(n_full), jnp.where(ids < n_left, s, -jnp.inf))

        s0[...] = scores(0, BLOCK_K)

        def pair(i, carry):
            j = 2 * i
            s1[...] = scores(base_of(j + 1), BLOCK_K)
            update(base_of(j), s0[...])
            s0[...] = scores(base_of(j + 2), BLOCK_K)
            update(base_of(j + 1), s1[...])
            return carry

        lax.fori_loop(0, n_full // 2, pair, 0)
        odd = lax.rem(n_full, 2) == 1

        @pl.when(odd)
        def _():
            s1[...] = scores(base_of(n_full), BLOCK_K)
            update(base_of(n_full - 1), s0[...])

            @pl.when(n_left > 0)
            def _():
                update_last(s1[...])

        @pl.when(jnp.logical_not(odd) & (n_left > 0))
        def _():
            update_last(s0[...])

    if use_new:
        piece = me ^ (first + qi)

        def new_base(j):
            return pl.multiple_of(n_cache + j * n_rows, 256)

        def earlier(j, carry):
            update(new_base(j), scores(new_base(j), n_rows))
            return carry

        lax.fori_loop(0, piece, earlier, 0)
        s = scores(new_base(piece), n_rows)
        key_ids = lax.broadcasted_iota(jnp.int32, s.shape, 0)
        row_ids = lax.broadcasted_iota(jnp.int32, s.shape, 1)
        update(new_base(piece), jnp.where(key_ids <= row_ids, s, -jnp.inf))

    if store:
        m_out[...], l_out[...], acc_out[...] = m_s[...], l_s[...], acc_s[...]
    else:
        result = (acc_s[...] / l_s[...]).T.astype(jnp.bfloat16)
        for i, o_ref in enumerate(outs):
            @pl.when(qi == i)
            def _():
                o_ref[...] = result


def global_attention(info, q, cache_k=(), cache_v=(), new_k=(), new_v=(), state=(), first=0, store=False, n_dev=4):
    dim = HEAD_DIM
    n_rows, group = q.shape[0] // 2, q.shape[1]
    heads = group // dim
    slots = cache_k[0].shape[1] if cache_k else 0
    n_keys = n_dev * (slots + (n_rows if new_k else 0))
    elems = heads * 2 * n_rows * (n_dev * slots * 3 // 4 + (n_dev * n_rows // 2 if new_k else 0))
    state_specs = [pl.BlockSpec((None, None, r, n_rows), lambda h, i, m: (h, i, 0, 0)) for r in (1, 1, dim)]
    state_shape = [jax.ShapeDtypeStruct((heads, 2, r, n_rows), jnp.float32) for r in (1, 1, dim)]
    return pl.pallas_call(
        functools.partial(global_kernel, n_dev=n_dev, slots=slots, n_rows=n_rows, first=first, use_cache=bool(cache_k), use_new=bool(new_k), load=bool(state), store=store),
        grid_spec=pltpu.PrefetchScalarGridSpec(
            num_scalar_prefetch=1,
            grid=(heads, 2),
            in_specs=[pl.BlockSpec((n_rows, dim), lambda h, i, m: (i, h))] + [ANY] * (2 * len(cache_k) + 2 * len(new_k)) + (state_specs if state else []),
            out_specs=state_specs if store else [pl.BlockSpec((n_rows, dim), lambda h, i, m: (0, h))] * 2,
            scratch_shapes=[
                pltpu.VMEM((2, n_keys, dim), jnp.bfloat16),
                pltpu.VMEM((2, n_keys, dim), jnp.bfloat16),
                pltpu.VMEM((BLOCK_K, n_rows), jnp.float32),
                pltpu.VMEM((BLOCK_K, n_rows), jnp.float32),
                pltpu.VMEM((dim, n_rows), jnp.bfloat16),
                pltpu.VMEM((1, n_rows), jnp.float32),
                pltpu.VMEM((1, n_rows), jnp.float32),
                pltpu.VMEM((dim, n_rows), jnp.float32),
                pltpu.SemaphoreType.DMA((2, 2, n_dev + 4)),
            ],
        ),
        out_shape=state_shape if store else [jax.ShapeDtypeStruct((n_rows, group), jnp.bfloat16)] * 2,
        compiler_params=pltpu.CompilerParams(vmem_limit_bytes=56 << 20),
        cost_estimate=pl.CostEstimate(flops=8 * elems * dim, bytes_accessed=4 * heads * n_keys * dim, transcendentals=elems),
        name="global_attention",
    )(info, q, *cache_k, *cache_v, *new_k, *new_v, *state)


def local_kernel(q_ref, k_ref, v_ref, hk_ref, hv_ref, o_ref, kbuf, vbuf, *, window):
    n_rows = q_ref.shape[0]
    dim = HEAD_DIM
    key_ids = lax.broadcasted_iota(jnp.int32, (2 * window, window), 0)
    row_ids = lax.broadcasted_iota(jnp.int32, (2 * window, window), 1)
    allowed = (key_ids > row_ids) & (key_ids <= row_ids + window)
    kbuf[pl.ds(0, window), :] = hk_ref[...]
    kbuf[pl.ds(window, n_rows), :] = k_ref[...]
    vbuf[pl.ds(0, window), :] = hv_ref[...]
    vbuf[pl.ds(window, n_rows), :] = v_ref[...]
    for h in range(q_ref.shape[1] // dim):
        cols = pl.ds(h * dim, dim)
        for b in range(n_rows // window):
            keys = pl.ds(b * window, 2 * window)
            rows = pl.ds(b * window, window)
            s = lax.dot_general(kbuf[keys, cols], q_ref[rows, cols], NT, preferred_element_type=jnp.float32)
            s = jnp.where(allowed, s, -jnp.inf)
            probs = jnp.exp2((s - jnp.max(s, axis=0, keepdims=True)) * EXP_SCALE)
            total = jnp.sum(probs, axis=0, keepdims=True)
            o = lax.dot_general(vbuf[keys, cols], probs.astype(jnp.bfloat16), TN, preferred_element_type=jnp.float32)
            o_ref[rows, cols] = (o / total).T.astype(jnp.bfloat16)


def local_attention(q, k, v, halo_k, halo_v):
    n_rows, width = q.shape
    window = halo_k.shape[0]
    cols = 512
    row_spec = pl.BlockSpec((n_rows, cols), lambda h: (0, h))
    halo_spec = pl.BlockSpec((window, cols), lambda h: (0, h))
    elems = n_rows * 2 * window * (width // HEAD_DIM)
    return pl.pallas_call(
        functools.partial(local_kernel, window=window),
        grid=(width // cols,),
        in_specs=[row_spec, row_spec, row_spec, halo_spec, halo_spec],
        out_specs=row_spec,
        out_shape=jax.ShapeDtypeStruct((n_rows, width), jnp.bfloat16),
        scratch_shapes=[pltpu.VMEM((window + n_rows, cols), jnp.bfloat16)] * 2,
        compiler_params=pltpu.CompilerParams(vmem_limit_bytes=32 << 20),
        cost_estimate=pl.CostEstimate(flops=8 * elems * HEAD_DIM, bytes_accessed=8 * n_rows * width, transcendentals=elems),
        name="local_attention",
    )(q, k, v, halo_k, halo_v)


def solution(mesh):
    n_dev = mesh.shape['ctx']
    shift_pairs = [(src_dev, src_dev + 1) for src_dev in range(n_dev - 1)]
    row_spec = P(('dp', 'ctx'), None)
    cache_spec = P(None, ('dp', 'ctx'), None, None)
    local_spec = P(None, 'dp', None, None)
    in_specs = (row_spec, P('dp'), cache_spec, cache_spec, local_spec, local_spec) + (P(),) * 9

    def swap(x, r):
        return lax.ppermute(x, 'ctx', [(d, d ^ r) for d in range(n_dev)])

    def device_step(x_rows, cache_len, k_cache, v_cache, k_local, v_local, g_attn, g_mlp, w_q, w_k, w_v, w_o, w_gate, w_up, w_down):
        dev_idx = lax.axis_index('ctx')
        is_first = dev_idx == 0
        me = dev_idx.astype(jnp.int32).reshape(1)
        info = jnp.concatenate([me, cache_len])
        n_rows = x_rows.shape[0]
        pairs, window = k_local.shape[:2]
        width = w_q.shape[-1]
        halo_keys = k_local.reshape(pairs, window, width)
        halo_vals = v_local.reshape(pairs, window, width)
        sent = {}

        def relay_both(p):
            return relay(me, k_cache, p, n_dev), relay(me, v_cache, p, n_dev)

        def send(p, t, pieces):
            sent[p, t] = [pieces[0]] + [swap(pieces[r], r) for r in (1, 2, 3)]

        k_pieces, v_pieces = relay_both(0)
        x_rows, k_pieces = lax.optimization_barrier((x_rows, k_pieces))
        send(0, 'k', k_pieces)
        send(0, 'v', v_pieces)

        mlp_args = (w_o, g_mlp.reshape(2 * pairs, 1, width), w_gate, w_up, w_down)
        attn_gains = g_attn.reshape(2 * pairs, 1, width)
        hidden = x_rows
        h = rms_norm(hidden, g_attn[0])
        for p in range(pairs):
            l = 2 * p
            k = project(h, w_k[l])
            v = project(h, w_v[l])
            halo_k = lax.ppermute(k[n_rows - window:], 'ctx', shift_pairs)
            halo_v = lax.ppermute(v[n_rows - window:], 'ctx', shift_pairs)
            q = project(h, w_q[l])
            halo_k = jnp.where(is_first, halo_keys[p], halo_k)
            halo_v = jnp.where(is_first, halo_vals[p], halo_v)
            attn = local_attention(q, k, v, halo_k, halo_v)
            hidden, h = out_mlp(me, hidden, (attn,), *mlp_args, l, attn_gains)

            l = 2 * p + 1
            h1 = swap(h, 1)
            h2 = swap(h, 2)
            q_near, k_near, v_near = group_qkv(me, h, h1, w_q, w_k, w_v, l, n_dev)
            state = global_attention(info, q_near, sent[p, 'k'], sent[p, 'v'], store=True)
            h3 = swap(h2, 1)
            q_far, k_far, v_far = group_qkv(me, h2, h3, w_q, w_k, w_v, l, n_dev)
            if p + 1 < pairs:
                k_pieces, v_pieces = relay_both(p + 1)
                k_pieces, v_pieces = lax.optimization_barrier((k_pieces, v_pieces, q_far))[:2]
                send(p + 1, 'k', k_pieces)
            o2, o3 = global_attention(info, q_far, sent[p, 'k'], sent[p, 'v'], (k_near, k_far), (v_near, v_far), first=2)
            o2, o3 = swap(o2, 2), swap(o3, 3)
            if p + 1 < pairs:
                send(p + 1, 'v', v_pieces)
            o0, o1 = global_attention(info, q_near, (), (), (k_near, k_far), (v_near, v_far), state)
            o1 = swap(o1, 1)
            if p + 1 < pairs:
                hidden, h = out_mlp(me, hidden, (o0, o1, o2, o3), *mlp_args, l, attn_gains)
            else:
                hidden = out_mlp(me, hidden, (o0, o1, o2, o3), *mlp_args, l)
        return hidden

    return jax.shard_map(device_step, mesh=mesh, in_specs=in_specs, out_specs=row_spec, check_vma=False)
```
